1024 devices in a mesh: aa: 16 (over y, x_hi, core), ba: 64 (over x_lo, z).
Axes of the slice: x: 4 (x_hi: 2, x_lo: 2; x = x_hi * 2 + x_lo), y: 4, z: 32, core: 2. Of those that a mesh axis runs over, the one named last changes fastest.
Arguments:
- state: float32 [14, 64, 64, 128], P(None, 'ba', 'aa'), as said below
- labels: int32 [64, 64, 128], P('ba', 'aa'), may hold values from 0 to 2, as said below
Outputs:
- swept: float32 [14, 64, 64, 128], P(None, 'ba', 'aa')
The draws below stay inside these ranges and needn't reach their ends.
Inputs may be any that keep to these rules, and one draw needn't show every extreme that they name: `labels`: void cells lie in a band of low y and in scattered pores; projectile cells form one box inside the band. `state`: density is positive; inverse deformation gradients lie within 0.6 of the identity in every entry.
All inputs are finite; a program needn't handle non-finite values.
Results may differ from the reference program's by a relative error of at most 0.0003.
Values sent between devices are 32-bit elements; how exact they have to be, the bound alone decides.
A program may use at most 32 MiB of HBM per device.

```python
import jax
import jax.numpy as jnp
from jax import lax

NX = 128
RETURN_ITERS = 2
NY = 64
NZ = 64


GAMMA_TABLE = (3.0, 4.0, 1.4)


STIFF_TABLE = (1.0, 6.0, 0.0)


SHEAR_TABLE = (0.6, 3.0, 0.0)


def layout(key):
    zone = jax.random.fold_in(key, 11)
    keys = jax.random.split(zone, 4)
    depth = jax.random.randint(keys[0], (), NY // 4, NY // 2 + 1)
    tall = max(NY // 8, 2)
    broad = max(NX // 8, 2)
    top = jax.random.randint(keys[1], (), 0, depth - tall + 1)
    start = jax.random.randint(keys[2], (), 0, NX - broad + 1)
    row_index = lax.broadcasted_iota(jnp.int32, (NZ, NY, NX), 1)
    column_index = lax.broadcasted_iota(jnp.int32, (NZ, NY, NX), 2)
    pores = jax.random.randint(keys[3], (NZ, NY, NX), 0, 8) == 0
    inside = (row_index >= top) & (row_index < top + tall) & (column_index >= start) & (column_index < start + broad)
    return jnp.where(inside, 1, jnp.where((row_index < depth) | pores, 2, 0)).astype(jnp.int32)


def draw_labels(key, part):
    return layout(key)


def draw_state(key, part):
    labels = layout(key)
    sandy = labels == 0
    solid = labels == 1
    shape = (NZ, NY, NX)
    keys = jax.random.split(jax.random.fold_in(key, 23), 8)

    def spread(subkey, low, high):
        return jnp.exp(jax.random.uniform(subkey, shape, jnp.float32, jnp.log(low), jnp.log(high)))

    def pick(table):
        return jnp.where(sandy, table[0], jnp.where(solid, table[1], table[2]))
    density = jnp.where(sandy, spread(keys[0], 1.2, 2.4), jnp.where(solid, spread(keys[1], 6.0, 9.0), spread(keys[2], 0.05, 0.3)))
    pressure = spread(keys[3], 0.5, 2.0)
    velocity = 0.2 * jax.random.normal(keys[4], (3,) + shape, jnp.float32)
    faint = (labels == 2) & (jax.random.randint(keys[6], shape, 0, 8) == 0)
    pressure = jnp.where(faint, spread(keys[7], 0.01, 0.08), pressure)
    velocity = velocity.at[1].add(jnp.where(solid, 3.0, 0.0))
    amplitude = jnp.where(labels == 2, 0.02, 0.08)
    noise = jnp.clip(jax.random.normal(keys[5], (9,) + shape, jnp.float32), -6.0, 6.0) * amplitude
    gradient = [[noise[3 * row + col] + (1.0 if row == col else 0.0) for col in range(3)] for row in range(3)]
    metric = [[sum((gradient[row][first] * gradient[row][second] for row in range(3))) for second in range(3)] for first in range(3)]
    third = (metric[0][0] + metric[1][1] + metric[2][2]) / 3.0
    shear = pick(SHEAR_TABLE)
    elastic = 0.25 * shear * sum(((metric[first][second] - (third if first == second else 0.0)) ** 2 for first in range(3) for second in range(3)))
    gamma = pick(GAMMA_TABLE)
    stiff = pick(STIFF_TABLE)
    kinetic = 0.5 * density * (velocity[0] ** 2 + velocity[1] ** 2 + velocity[2] ** 2)
    total = kinetic + elastic + (pressure + gamma * stiff) / (gamma - 1.0)
    fields = [density] + [density * velocity[comp] for comp in range(3)] + [total] + [gradient[row][col] for row in range(3) for col in range(3)]
    return jnp.stack(fields).astype(jnp.float32)


def setup_inputs(seed: int = 0) -> dict:
    streams_of = jax.random.split(jax.random.key(seed), 3)
    return {
        "state": draw_state(jax.random.fold_in(streams_of[2], 71), 0),
        "labels": draw_labels(jax.random.fold_in(streams_of[2], 71), 0),
    }


GAMMA_TABLE = (3.0, 4.0, 1.4)
STIFF_TABLE = (1.0, 6.0, 0.0)
SHEAR_TABLE = (0.6, 3.0, 0.0)
COHESION_TABLE = (0.05, 0.0, 0.0)
FRICTION_TABLE = (0.4, 0.0, 0.0)
DENSITY_FLOOR = 0.2
TRACTION_FLOOR = 0.1
COURANT = 0.4
WENO_EPSILON = 1e-06

def material(label):

    def pick(table):
        return jnp.where(label == 0, table[0], jnp.where(label == 1, table[1], table[2]))
    return (pick(GAMMA_TABLE), pick(STIFF_TABLE), pick(SHEAR_TABLE), pick(COHESION_TABLE), pick(FRICTION_TABLE))

def deviator(gradient, shear):
    metric = [[sum((gradient[row][first] * gradient[row][second] for row in range(3))) for second in range(3)] for first in range(3)]
    third = (metric[0][0] + metric[1][1] + metric[2][2]) / 3.0
    devs = [[metric[first][second] - (third if first == second else 0.0) for second in range(3)] for first in range(3)]
    stress = [[-shear * devs[first][second] for second in range(3)] for first in range(3)]
    energy = 0.25 * shear * sum((devs[first][second] * devs[first][second] for first in range(3) for second in range(3)))
    return (stress, energy)

def primitives(fields, label):
    gamma, stiff, shear, cohesion, friction = material(label)
    density = jnp.maximum(fields[0], DENSITY_FLOOR)
    velocity = [fields[1 + comp] / density for comp in range(3)]
    gradient = [[fields[5 + 3 * row + col] for col in range(3)] for row in range(3)]
    stress, energy = deviator(gradient, shear)
    kinetic = 0.5 * (fields[1] * velocity[0] + fields[2] * velocity[1] + fields[3] * velocity[2])
    pressure = (gamma - 1.0) * (fields[4] - kinetic - energy) - gamma * stiff
    sound = jnp.sqrt((gamma * jnp.maximum(pressure + stiff, TRACTION_FLOOR) + 4.0 / 3.0 * shear) / density)
    return (density, velocity, gradient, stress, pressure, sound)

def weno_face(first, second, centre, fourth, fifth):
    cand_a = (2.0 * first - 7.0 * second + 11.0 * centre) / 6.0
    cand_b = (-second + 5.0 * centre + 2.0 * fourth) / 6.0
    cand_c = (2.0 * centre + 5.0 * fourth - fifth) / 6.0
    rough_a = 13.0 / 12.0 * (first - 2.0 * second + centre) ** 2 + 0.25 * (first - 4.0 * second + 3.0 * centre) ** 2
    rough_b = 13.0 / 12.0 * (second - 2.0 * centre + fourth) ** 2 + 0.25 * (second - fourth) ** 2
    rough_c = 13.0 / 12.0 * (centre - 2.0 * fourth + fifth) ** 2 + 0.25 * (3.0 * centre - 4.0 * fourth + fifth) ** 2
    weight_a = 0.1 / (WENO_EPSILON + rough_a) ** 2
    weight_b = 0.6 / (WENO_EPSILON + rough_b) ** 2
    weight_c = 0.3 / (WENO_EPSILON + rough_c) ** 2
    return (weight_a * cand_a + weight_b * cand_b + weight_c * cand_c) / (weight_a + weight_b + weight_c)

def riemann(left_fields, right_fields, left_label, right_label, direction):
    left = primitives(left_fields, left_label)
    right = primitives(right_fields, right_label)
    left_speed = left[1][direction]
    right_speed = right[1][direction]
    slow = jnp.minimum(left_speed - left[5], right_speed - right[5])
    fast = jnp.maximum(left_speed + left[5], right_speed + right[5])
    left_traction = left[4] - left[3][direction][direction]
    right_traction = right[4] - right[3][direction][direction]
    left_gap = slow - left_speed
    right_gap = fast - right_speed
    contact = (right_traction - left_traction + left[0] * left_speed * left_gap - right[0] * right_speed * right_gap) / (left[0] * left_gap - right[0] * right_gap)
    margin = 0.05 * (fast - slow)
    contact = jnp.clip(contact, slow + margin, fast - margin)

    def conserved(fields, prim):
        return [prim[0], fields[1], fields[2], fields[3], fields[4]]

    def normal_flux(fields, prim, traction):
        speed = prim[1][direction]
        out = [fields[1 + direction]]
        for comp in range(3):
            out.append(fields[1 + comp] * speed + (traction if comp == direction else 0.0))
        out.append((fields[4] + traction) * speed)
        return out

    def star(fields, prim, wave, gap, traction):
        ratio = gap / (wave - contact)
        mass = prim[0] * ratio
        moment = [mass * contact if comp == direction else mass * prim[1][comp] for comp in range(3)]
        energy = ratio * (fields[4] + (contact - prim[1][direction]) * (prim[0] * contact + traction / gap))
        return [mass] + moment + [energy]
    flux_left = normal_flux(left_fields, left, left_traction)
    flux_right = normal_flux(right_fields, right, right_traction)
    state_left = conserved(left_fields, left)
    state_right = conserved(right_fields, right)
    star_left = star(left_fields, left, slow, left_gap, left_traction)
    star_right = star(right_fields, right, fast, right_gap, right_traction)
    result = []
    for comp in range(5):
        through_left = flux_left[comp] + slow * (star_left[comp] - state_left[comp])
        through_right = flux_right[comp] + fast * (star_right[comp] - state_right[comp])
        result.append(jnp.where(slow >= 0, flux_left[comp], jnp.where(contact >= 0, through_left, jnp.where(fast > 0, through_right, flux_right[comp]))))
    for comp in range(3):
        if comp != direction:
            result[1 + comp] = result[1 + comp] - 0.5 * (left[3][comp][direction] + right[3][comp][direction])
            result[4] = result[4] - 0.5 * (left[3][direction][comp] * left[1][comp] + right[3][direction][comp] * right[1][comp])
    for row in range(3):
        flow_left = sum((left[2][row][comp] * left[1][comp] for comp in range(3)))
        flow_right = sum((right[2][row][comp] * right[1][comp] for comp in range(3)))
        jump = right_fields[5 + 3 * row + direction] - left_fields[5 + 3 * row + direction]
        blended = (fast * flow_left - slow * flow_right + slow * fast * jump) / (fast - slow)
        result.append(jnp.where(slow >= 0, flow_left, jnp.where(fast <= 0, flow_right, blended)))
    return result

def plastic(fields, label):
    gamma, stiff, shear, cohesion, friction = material(label)
    prim = primitives(fields, label)
    sandy = label == 0
    radius = jnp.where(sandy, cohesion + friction * jnp.maximum(prim[4], 0.0), 1.0)
    gradient = prim[2]
    for turn in range(RETURN_ITERS):
        stress, unused = deviator(gradient, shear)
        norm = jnp.sqrt(sum((stress[row][col] * stress[row][col] for row in range(3) for col in range(3))))
        factor = jnp.where(sandy, 0.5 * (1.0 + radius / jnp.maximum(norm, radius)), 1.0)
        third = (gradient[0][0] + gradient[1][1] + gradient[2][2]) / 3.0
        gradient = [[factor * gradient[row][col] + ((1.0 - factor) * third if row == col else 0.0) for col in range(3)] for row in range(3)]
    return fields[:5] + [gradient[row][col] for row in range(3) for col in range(3)]

def sweep(padded, label_pad, axis, direction, step_size):
    cells = padded.shape[axis] - 6
    faces = cells + 1

    def part(array, offset, count):
        return lax.slice_in_dim(array, offset, offset + count, axis=axis)
    shifted = [part(padded, offset, faces) for offset in range(6)]
    left_state = weno_face(shifted[0], shifted[1], shifted[2], shifted[3], shifted[4])
    right_state = weno_face(shifted[5], shifted[4], shifted[3], shifted[2], shifted[1])
    left_label = part(label_pad, 2, faces)[0]
    right_label = part(label_pad, 3, faces)[0]
    fluxes = riemann([left_state[comp] for comp in range(14)], [right_state[comp] for comp in range(14)], left_label, right_label, direction)
    centre = part(padded, 3, cells)
    label = part(label_pad, 3, cells)[0]
    fields = [centre[comp] for comp in range(14)]
    changed = [0, 1, 2, 3, 4] + [5 + 3 * row + direction for row in range(3)]
    for slot in range(8):
        flux = fluxes[slot]
        change = lax.slice_in_dim(flux, 1, faces, axis=axis - 1) - lax.slice_in_dim(flux, 0, cells, axis=axis - 1)
        fields[changed[slot]] = fields[changed[slot]] - step_size * change
    return jnp.stack(plastic(fields, label))

def edge_pad(array, axis):
    widths = [(0, 0)] * array.ndim
    widths[axis] = (3, 3)
    return jnp.pad(array, widths, mode='edge')

def peak_speed(state, label):
    prim = primitives([state[comp] for comp in range(14)], label)
    fastest = jnp.maximum(jnp.maximum(jnp.abs(prim[1][0]), jnp.abs(prim[1][1])), jnp.abs(prim[1][2]))
    return jnp.max(fastest + prim[5])

def reference(state, labels):
    step_size = COURANT / peak_speed(state, labels)
    label_block = labels[None]

    def along(current, moved_dim, axis, direction):
        moved = jnp.moveaxis(current, moved_dim, 0)
        moved_labels = jnp.moveaxis(label_block, moved_dim, 0)

        def single(pair):
            slab, label_slab = pair
            return sweep(edge_pad(slab, axis), edge_pad(label_slab, axis), axis, direction, step_size)
        return jnp.moveaxis(lax.map(single, (moved, moved_labels)), 0, moved_dim)
    after_x = along(state, 1, 2, 0)
    after_y = along(after_x, 1, 1, 1)
    return along(after_y, 2, 1, 2)
```

```python
import jax
import jax.numpy as jnp
from jax import lax
from jax.experimental import pallas as pl
from jax.experimental.pallas import tpu as pltpu
from jax.sharding import PartitionSpec as P

MESH = pl.DeviceIdType.MESH
COURANT = 0.4
EPS = 1e-06
NA, NB, NZC = 16, 64, 32
REACH = 8
ROWS = 80
F32 = jnp.float32


def pick(label, sand, solid, void):
    return jnp.where(label == 0.0, sand, jnp.where(label == 1.0, solid, void))


def deviator(g):
    def dot(i, j):
        return g[i] * g[j] + g[3 + i] * g[3 + j] + g[6 + i] * g[6 + j]

    xx, yy, zz = dot(0, 0), dot(1, 1), dot(2, 2)
    third = (xx + yy + zz) * (1.0 / 3.0)
    return (xx - third, yy - third, zz - third, dot(0, 1), dot(0, 2), dot(1, 2))


def squares(dev):
    return (
        dev[0] * dev[0]
        + dev[1] * dev[1]
        + dev[2] * dev[2]
        + 2.0 * (dev[3] * dev[3] + dev[4] * dev[4] + dev[5] * dev[5])
    )


def primitives(fields, label):
    gamma = pick(label, 3.0, 4.0, 1.4)
    stiff = pick(label, 1.0, 6.0, 0.0)
    shear = pick(label, 0.6, 3.0, 0.0)
    density = jnp.maximum(fields[0], 0.2)
    inverse = 1.0 / density
    velocity = [fields[1 + k] * inverse for k in range(3)]
    dev = deviator(fields[5:14])
    energy = 0.25 * shear * squares(dev)
    kinetic = 0.5 * (
        fields[1] * velocity[0] + fields[2] * velocity[1] + fields[3] * velocity[2]
    )
    pressure = (gamma - 1.0) * (fields[4] - kinetic - energy) - gamma * stiff
    sound = jnp.sqrt(
        (gamma * jnp.maximum(pressure + stiff, 0.1) + (4.0 / 3.0) * shear) * inverse
    )
    return density, velocity, dev, shear, pressure, sound


OFF = {(0, 1): 3, (1, 0): 3, (0, 2): 4, (2, 0): 4, (1, 2): 5, (2, 1): 5}


def riemann(left, right, label_left, label_right, d):
    rl, ul, dl, ml, pl_, cl = primitives(left, label_left)
    rr, ur, dr, mr, pr, cr = primitives(right, label_right)
    slow = jnp.minimum(ul[d] - cl, ur[d] - cr)
    fast = jnp.maximum(ul[d] + cl, ur[d] + cr)
    tl = pl_ + ml * dl[d]
    tr = pr + mr * dr[d]
    gl = slow - ul[d]
    gr = fast - ur[d]
    al = rl * gl
    ar = rr * gr
    contact = (tr - tl + al * ul[d] - ar * ur[d]) / (al - ar)
    margin = 0.05 * (fast - slow)
    contact = jnp.minimum(jnp.maximum(contact, slow + margin), fast - margin)
    is_left = contact >= 0.0

    def side(x, y):
        return jnp.where(is_left, x, y)

    r = side(rl, rr)
    m = [side(left[1 + k], right[1 + k]) for k in range(3)]
    e = side(left[4], right[4])
    u = side(ul[d], ur[d])
    t = side(tl, tr)
    wave = side(slow, fast)
    gap = side(gl, gr)
    active = jnp.where(is_left, -slow, fast) > 0.0
    over = 1.0 / (wave - contact)
    chi = gap * over
    mass = r * chi
    energy = chi * (e + (contact - u) * (r * contact)) + (contact - u) * t * over
    jump = [mass - r]
    for k in range(3):
        jump.append(mass * contact - m[k] if k == d else chi * m[k] - m[k])
    jump.append(energy - e)
    flux = [m[d]]
    for k in range(3):
        flux.append(m[k] * u + t if k == d else m[k] * u)
    flux.append((e + t) * u)
    out = [flux[k] + jnp.where(active, wave * jump[k], 0.0) for k in range(5)]
    hl, hr = 0.5 * ml, 0.5 * mr
    for k in range(3):
        if k != d:
            o = OFF[(k, d)]
            sl, sr = hl * dl[o], hr * dr[o]
            out[1 + k] = out[1 + k] + (sl + sr)
            out[4] = out[4] + (sl * ul[k] + sr * ur[k])
    span = 1.0 / (fast - slow)
    both = slow * fast
    for i in range(3):
        b = 5 + 3 * i
        fl = left[b] * ul[0] + left[b + 1] * ul[1] + left[b + 2] * ul[2]
        fr = right[b] * ur[0] + right[b + 1] * ur[1] + right[b + 2] * ur[2]
        mix = (fast * fl - slow * fr + both * (right[b + d] - left[b + d])) * span
        out.append(jnp.where(slow >= 0.0, fl, jnp.where(fast <= 0.0, fr, mix)))
    return out


def plastic(fields, label):
    sandy = label == 0.0
    g = fields[5:14]
    dev = deviator(g)
    sq = squares(dev)
    kinetic = (
        0.5
        * (fields[1] * fields[1] + fields[2] * fields[2] + fields[3] * fields[3])
        / jnp.maximum(fields[0], 0.2)
    )
    pressure = 2.0 * (fields[4] - kinetic - 0.15 * sq) - 3.0
    radius = 0.05 + 0.4 * jnp.maximum(pressure, 0.0)
    cur = g
    for turn in range(2):
        if turn:
            sq = squares(deviator(cur))
        norm = 0.6 * jnp.sqrt(sq)
        factor = 0.5 * (1.0 + radius / jnp.maximum(norm, radius))
        shift = (1.0 - factor) * ((cur[0] + cur[4] + cur[8]) * (1.0 / 3.0))
        cur = [factor * cur[k] + shift if k % 4 == 0 else factor * cur[k] for k in range(9)]
    return list(fields[:5]) + [jnp.where(sandy, cur[k], g[k]) for k in range(9)]


def smooth(d1, d2, d3, d4):
    s1, s2, s3 = d2 - d1, d3 - d2, d4 - d3
    w1, w2, w3 = 3.0 * d2 - d1, d2 + d3, d4 - 3.0 * d3
    c = 13.0 / 12.0
    qa = 1.0 / (EPS + c * (s1 * s1) + 0.25 * (w1 * w1))
    qb = 1.0 / (EPS + c * (s2 * s2) + 0.25 * (w2 * w2))
    qc = 1.0 / (EPS + c * (s3 * s3) + 0.25 * (w3 * w3))
    return qa * qa, 6.0 * (qb * qb), qc * qc


def weno_plus(q, d1, d2, d3, d4):
    qa, qb, qc = q
    qc = 3.0 * qc
    top = qa * (5.0 * d2 - 2.0 * d1) + qb * (d2 + 2.0 * d3) + qc * (4.0 * d3 - d4)
    return top / (6.0 * (qa + qb + qc))


def weno_minus(q, d1, d2, d3, d4):
    qa, qb, qc = q
    qa = 3.0 * qa
    top = qc * (2.0 * d4 - 5.0 * d3) - qb * (d3 + 2.0 * d2) + qa * (d1 - 4.0 * d2)
    return top / (6.0 * (qa + qb + qc))


def end_delta(d):
    t = 1.0 / (1.0 + (4.0 / 3.0 / EPS) * (d * d))
    t = t * t
    return d * (0.05 * t) / (0.7 + 0.3 * t)


def lane_iota(shape):
    return lax.broadcasted_iota(jnp.int32, shape, len(shape) - 1)


def changed(d):
    return [0, 1, 2, 3, 4] + [5 + 3 * i + d for i in range(3)]


def row(r):
    if isinstance(r, int):
        return pl.ds(r * 8, 8)
    return pl.ds(pl.multiple_of(r * 8, 8), 8)


def x_faces(source, r, flux_ref, ends_left, ends_right, slot):
    lane = lane_iota((8, 128))
    first, last = lane == 0, lane == 127
    here = lane == slot
    left, right = [], []
    for f in range(14):
        s = source(f)
        up = jnp.where(last, 0.0, pltpu.roll(s, 127, 1) - s)
        d3 = up
        d2 = pltpu.roll(up, 1, 1)
        d1 = jnp.where(first, 0.0, pltpu.roll(up, 2, 1))
        d4 = jnp.where(last, 0.0, pltpu.roll(up, 127, 1))
        q = smooth(d1, d2, d3, d4)
        plus = s + weno_plus(q, d1, d2, d3, d4)
        minus = s + weno_minus(q, d1, d2, d3, d4)
        g = end_delta(jnp.where(last, d2, up))
        left.append(jnp.where(first, s - g, pltpu.roll(plus, 1, 1)))
        right.append(minus)
        ends_left[f] = jnp.where(here, plus[:, 127:128], ends_left[f])
        ends_right[f] = jnp.where(here, (s + g)[:, 127:128], ends_right[f])
    label = source(14)
    ends_left[14] = jnp.where(here, label[:, 127:128], ends_left[14])
    label_left = jnp.where(first, label, pltpu.roll(label, 1, 1))
    fluxes = riemann(left, right, label_left, label, 0)
    for k in range(8):
        flux_ref[k, row(slot)] = fluxes[k]


def x_ends(ends_left, ends_right, end_flux):
    left = [ends_left[f] for f in range(14)]
    right = [ends_right[f] for f in range(14)]
    label = ends_left[14]
    fluxes = riemann(left, right, label, label, 0)
    for k in range(8):
        end_flux[k] = fluxes[k]


def x_update(source, r, flux_ref, end_flux, step, after):
    lane = lane_iota((8, 128))
    last = lane == 127
    fields = [source(f) for f in range(14)]
    for k, f in enumerate(changed(0)):
        flux = flux_ref[k, row(r)]
        end = jnp.sum(jnp.where(lane == r, end_flux[k], 0.0), axis=1, keepdims=True)
        upper = jnp.where(last, end, pltpu.roll(flux, 127, 1))
        fields[f] = fields[f] - step * (upper - flux)
    fields = plastic(fields, source(14))
    for f in range(14):
        after[f, row(r)] = fields[f]


def y_states(after, c, plus_ref, minus_ref):
    for f in range(14):
        s = [after[f, row(c + k)] for k in range(-2, 3)]
        d1, d2, d3, d4 = [s[k + 1] - s[k] for k in range(4)]
        q = smooth(d1, d2, d3, d4)
        plus_ref[f, row(c - 2)] = s[2] + weno_plus(q, d1, d2, d3, d4)
        minus_ref[f, row(c - 2)] = s[2] + weno_minus(q, d1, d2, d3, d4)


def y_flux(j, plus_ref, minus_ref, label_of, flux_ref):
    left = [plus_ref[f, row(j)] for f in range(14)]
    right = [minus_ref[f, row(j + 1)] for f in range(14)]
    fluxes = riemann(left, right, label_of(j + 2), label_of(j + 3), 1)
    for k in range(8):
        flux_ref[k, row(j)] = fluxes[k]


def y_update(j, after, label_of, flux_ref, step, done):
    fields = [after[f, row(j + 3)] for f in range(14)]
    for k, f in enumerate(changed(1)):
        fields[f] = fields[f] - step * (flux_ref[k, row(j + 1)] - flux_ref[k, row(j)])
    fields = plastic(fields, label_of(j + 3))
    for f in range(14):
        start = (f * 4 + j) * 8
        done[pl.ds(start, 8)] = fields[f]


def z_sweep(done, layer_label, step, out):
    low = lax.broadcasted_iota(jnp.int32, (8, 128), 0) < 4

    def swap(x):
        return pltpu.roll(x, 4, 0)

    left, right, centre = [], [], []
    for p in range(7):
        s = [done[pl.ds(p * 64 + o, 8, stride=8)] for o in range(7)]
        d = [s[k + 1] - s[k] for k in range(6)]
        q2 = smooth(*d[0:4])
        q3 = smooth(*d[1:5])
        q4 = smooth(*d[2:6])
        l_low = s[2] + weno_plus(q2, *d[0:4])
        r_low = s[3] + weno_minus(q3, *d[1:5])
        l_up = s[3] + weno_plus(q3, *d[1:5])
        r_up = s[4] + weno_minus(q4, *d[2:6])
        left += [jnp.where(low, l_low, swap(l_up)), jnp.where(low, swap(l_low), l_up)]
        right += [jnp.where(low, r_low, swap(r_up)), jnp.where(low, swap(r_low), r_up)]
        centre += [s[3], swap(s[3])]
    lab2, lab3, lab4 = layer_label(2), layer_label(3), layer_label(4)
    fluxes = riemann(
        left, right, jnp.where(low, lab2, swap(lab3)), jnp.where(low, lab3, swap(lab4)), 2
    )
    for k, f in enumerate(changed(2)):
        centre[f] = centre[f] - step * (swap(fluxes[k]) - fluxes[k])
    fields = plastic(centre, lab3)
    for f in range(14):
        out[f, 0] = fields[f][0:4]


def clamped(r, place):
    low = jnp.where(place == 0, 3, 0)
    high = jnp.where(place == NA - 1, 6, 9)
    return jnp.minimum(jnp.maximum(r, low), high)


def compute_body(place, halo, peak, out, flux_x, ends_left, ends_right, end_flux, after,
                 plus_ref, minus_ref, flux_y, done):
    step = COURANT / jnp.max(peak[...], keepdims=True)

    def source_of(r):
        at = row(clamped(r, place))
        return lambda f: halo[f, at]

    ends_left[...] = jnp.ones_like(ends_left)
    ends_right[...] = jnp.ones_like(ends_right)

    def faces(r, carry):
        x_faces(source_of(r), r, flux_x, ends_left, ends_right, r)
        return carry

    lax.fori_loop(0, 10, faces, 0)
    x_ends(ends_left, ends_right, end_flux)

    def update(r, carry):
        x_update(source_of(r), r, flux_x, end_flux, step, after)
        return carry

    lax.fori_loop(0, 10, update, 0)

    def states(i, carry):
        y_states(after, i + 2, plus_ref, minus_ref)
        return carry

    lax.fori_loop(0, 6, states, 0)

    def label_of(r):
        return source_of(r)(14)

    for j in range(5):
        y_flux(j, plus_ref, minus_ref, label_of, flux_y)
    for j in range(4):
        y_update(j, after, label_of, flux_y, step, done)

    def layer_label(o):
        return pltpu.roll(halo[14, pl.ds(o, 8, stride=8)], 5, 0)

    z_sweep(done, layer_label, step, out)


COMPUTE_SCRATCH = [
    pltpu.VMEM((8, ROWS, 128), F32),
    pltpu.VMEM((15, 8, 128), F32),
    pltpu.VMEM((14, 8, 128), F32),
    pltpu.VMEM((8, 8, 128), F32),
    pltpu.VMEM((14, ROWS, 128), F32),
    pltpu.VMEM((14, 48, 128), F32),
    pltpu.VMEM((14, 48, 128), F32),
    pltpu.VMEM((8, 40, 128), F32),
    pltpu.VMEM((448, 128), F32),
]


def compute_kernel(*refs):
    compute_body(lax.axis_index("aa"), *refs)


def gather_kernel(state, labels, halo, peak, layers, marks, m0, r1, m1, ra, m2, rb,
                  local_sem, z_send, z_recv, l_send, l_recv, y_send, y_recv, m_send, m_recv):
    a, b = lax.axis_index("aa"), lax.axis_index("ba")
    xl, z = b // NZC, b % NZC
    barrier = pltpu.get_barrier_semaphore()

    def plane(t):
        i = (a * 2 + xl + t) % (2 * NA)
        return (i // 2, (i % 2) * NZC + z)

    def ring(k):
        return (a, xl * NZC + (z + (k + NZC)) % NZC)

    def along(k):
        return (a, (b + (k + NB)) % NB)

    def across(k):
        return ((a + (k + NA)) % NA, b)

    def greet(device):
        pl.semaphore_signal(barrier, inc=1, device_id=device, device_id_type=MESH)

    near = (1, -1, 2, -2, 3, -3)
    for k in near:
        greet(along(k))

    def greet_plane(t, carry):
        greet(plane(t))
        return carry

    def greet_ring(k, carry):
        greet(ring(k))
        greet(ring(-k))
        return carry

    lax.fori_loop(1, REACH + 1, greet_ring, 0)
    lax.fori_loop(1, 2 * NA, greet_plane, 0)
    own_state = pltpu.make_async_copy(state.at[:, 0], layers.at[3], local_sem.at[0])
    own_label = pltpu.make_async_copy(labels.at[0], marks.at[3], local_sem.at[1])
    own_state.start()
    own_label.start()
    own_state.wait()
    own_label.wait()
    fields = [layers[3, f] for f in range(14)]
    label = marks[3].astype(F32)
    density, velocity, dev, shear, pressure, sound = primitives(fields, label)
    speed = sound + jnp.maximum(
        jnp.maximum(jnp.abs(velocity[0]), jnp.abs(velocity[1])), jnp.abs(velocity[2])
    )
    m0[...] = jnp.max(speed, axis=0, keepdims=True)
    pl.semaphore_wait(barrier, len(near) + 2 * REACH + 2 * NA - 1)

    def copy(src, dst, send, recv, device):
        return pltpu.make_async_remote_copy(
            src_ref=src, dst_ref=dst, send_sem=send, recv_sem=recv,
            device_id=device, device_id_type=MESH,
        )

    def send_plane(t, carry):
        copy(m0, r1.at[t - 1], m_send.at[0], m_recv.at[0], plane(t)).start()
        return carry

    lax.fori_loop(1, 2 * NA, send_plane, 0)
    z_copies = []
    for i, k in enumerate(near):
        z_copies.append(
            copy(layers.at[3], layers.at[3 - k], z_send.at[i], z_recv.at[i], along(k))
        )
        z_copies.append(
            copy(marks.at[3], marks.at[3 - k], l_send.at[i], l_recv.at[i], along(k))
        )
    for c in z_copies:
        c.start()
    all_plane = copy(r1, r1, m_send.at[0], m_recv.at[0], plane(1))
    all_plane.wait_recv()
    m1[...] = jnp.maximum(m0[...], jnp.max(r1[...], axis=0))

    def send_ring(k, carry):
        copy(m1, ra.at[k - 1], m_send.at[1], m_recv.at[1], ring(k)).start()
        copy(m1, ra.at[REACH + k - 1], m_send.at[1], m_recv.at[1], ring(-k)).start()
        return carry

    lax.fori_loop(1, REACH + 1, send_ring, 0)
    for c in z_copies:
        c.wait_recv()
    for slot in range(7):
        at = jnp.minimum(jnp.maximum(b + (slot - 3), 0), NB - 1) - b + 3
        for f in range(14):
            halo[f, pl.ds(24 + slot, 4, stride=8)] = layers[at, f]
        halo[14, pl.ds(24 + slot, 4, stride=8)] = marks[at].astype(F32)
    for f in range(15):
        halo[f, pl.ds(24 + 7, 4, stride=8)] = halo[f, pl.ds(24 + 6, 4, stride=8)]
    y_copies = [
        copy(halo.at[:, pl.ds(32, 24)], halo.at[:, pl.ds(0, 24)], y_send.at[0], y_recv.at[0], across(1)),
        copy(halo.at[:, pl.ds(24, 24)], halo.at[:, pl.ds(56, 24)], y_send.at[1], y_recv.at[1], across(-1)),
    ]
    for c in y_copies:
        c.start()
    all_ring = copy(ra, ra, m_send.at[1], m_recv.at[1], ring(1))
    all_ring.wait_recv()
    m2[...] = jnp.maximum(m1[...], jnp.max(ra[...], axis=0))
    far = [
        copy(m2, rb.at[0], m_send.at[2], m_recv.at[2], ring(REACH)),
        copy(m2, rb.at[1], m_send.at[3], m_recv.at[3], ring(-REACH)),
    ]
    for c in far:
        c.start()
    for c in y_copies:
        c.wait_recv()
    for c in far:
        c.wait_recv()
    total = jnp.maximum(m2[...], jnp.maximum(rb[0], rb[1]))
    peak[...] = jnp.broadcast_to(total, (8, 128))
    all_plane.wait_send()
    all_ring.wait_send()
    for c in z_copies + y_copies + far:
        c.wait_send()


GATHER_SCRATCH = [
    pltpu.VMEM((7, 14, 4, 128), F32),
    pltpu.VMEM((7, 4, 128), jnp.int32),
    pltpu.VMEM((1, 128), F32),
    pltpu.VMEM((2 * NA - 1, 1, 128), F32),
    pltpu.VMEM((1, 128), F32),
    pltpu.VMEM((2 * REACH, 1, 128), F32),
    pltpu.VMEM((1, 128), F32),
    pltpu.VMEM((2, 1, 128), F32),
    pltpu.SemaphoreType.DMA((2,)),
    pltpu.SemaphoreType.DMA((6,)),
    pltpu.SemaphoreType.DMA((6,)),
    pltpu.SemaphoreType.DMA((6,)),
    pltpu.SemaphoreType.DMA((6,)),
    pltpu.SemaphoreType.DMA((2,)),
    pltpu.SemaphoreType.DMA((2,)),
    pltpu.SemaphoreType.DMA((4,)),
    pltpu.SemaphoreType.DMA((4,)),
]

VM = pl.BlockSpec(memory_space=pltpu.VMEM)


def shards(state, labels):
    halo, peak = pl.pallas_call(
        gather_kernel,
        out_shape=[
            jax.ShapeDtypeStruct((15, ROWS, 128), F32),
            jax.ShapeDtypeStruct((8, 128), F32),
        ],
        in_specs=[pl.BlockSpec(memory_space=pl.ANY)] * 2,
        out_specs=[VM, VM],
        scratch_shapes=GATHER_SCRATCH,
        compiler_params=pltpu.CompilerParams(collective_id=0, has_side_effects=True),
        name="gather",
    )(state, labels)
    return pl.pallas_call(
        compute_kernel,
        out_shape=jax.ShapeDtypeStruct((14, 1, 4, 128), F32),
        in_specs=[VM, VM],
        out_specs=VM,
        scratch_shapes=COMPUTE_SCRATCH,
        name="compute",
    )(halo, peak)


def solution(mesh):
    return jax.shard_map(
        shards,
        mesh=mesh,
        in_specs=(P(None, "ba", "aa", None), P("ba", "aa", None)),
        out_specs=P(None, "ba", "aa", None),
        check_vma=False,
    )
```
